32 devices in a mesh: fsdp: 4 (over y, x), width: 8 (over z, core).
Axes of the slice: x: 2, y: 2, z: 4, core: 2. Of those that a mesh axis runs over, the one named last changes fastest.
Arguments:
- train_gate: float32 [4096, 11008], P('fsdp', 'width'), may hold values from -0.125 to 0.125
- drift_gate: float32 [4096, 11008], P('fsdp', 'width'), may hold values from -0.09375 to 0.09375
- spread_gate: float32 [4096, 11008], P('fsdp', 'width'), may hold values from -0.09375 to 0.09375
- train_up: float32 [4096, 11008], P('fsdp', 'width'), may hold values from -0.125 to 0.125
- drift_up: float32 [4096, 11008], P('fsdp', 'width'), may hold values from -0.09375 to 0.09375
- spread_up: float32 [4096, 11008], P('fsdp', 'width'), may hold values from -0.09375 to 0.09375
- norm_train: float32 [4096], P(('fsdp', 'width')), may hold values from 0.25 to 1.75
- norm_step: float32 [4096], P(('fsdp', 'width')), may hold values from -0.3 to 0.3
Outputs:
- serving_gate: bfloat16 [4096, 11008], P(None, 'width')
- serving_up: bfloat16 [4096, 11008], P(None, 'width')
- scale_gate: float32 [11008], P('width')
- scale_up: float32 [11008], P('width')
- serve_norm: bfloat16 [4096], replicated
- whole_gate: float32 [4096, 11008], P('fsdp', 'width')
- whole_up: float32 [4096, 11008], P('fsdp', 'width')
The draws below stay inside these ranges and needn't reach their ends.
All inputs are finite; a program needn't handle non-finite values.
Results may differ from the reference program's by a relative error of at most 0.0004.
Values may be sent and summed in bfloat16 or wider, within the bound.
A program may use at most 128 MiB of HBM per device.

```python
import jax
import jax.numpy as jnp
from jax import lax

D_MODEL = 4096
D_INNER = 11008


def strengthened(entries, key, source, target, shards_of, factor):
    def block_of(axis_at):
        return (jnp.arange(entries.shape[axis_at]) // (entries.shape[axis_at] // shards_of)).reshape((-1,) + (1,) * (entries.ndim - 1 - axis_at))

    one_side = jax.random.permutation(key, shards_of)[block_of(target)]
    other_side = (block_of(target) + shards_of // 2) % shards_of
    return jnp.where((block_of(source) == one_side) | (block_of(source) == other_side), factor * entries, entries)


def level_of(own_key, dims, split, smallest, largest):
    loudness = 1.0
    for position, parts in split:
        draws = jax.random.uniform(jax.random.fold_in(jax.random.fold_in(own_key, 6), position), (parts,), jnp.float32, smallest / len(split), largest / len(split))
        loudness = loudness * jnp.repeat(jnp.exp(draws), dims[position] // parts).reshape((-1,) + (1,) * (len(dims) - 1 - position))
    return loudness


def gaussian(own_key, dims, width, reach, cuts=(), held_as=jnp.bfloat16):
    array = width * jax.random.normal(own_key, dims, jnp.float32)
    if cuts:
        array = array * level_of(own_key, dims, cuts, -0.22, 0.18)
    return jnp.clip(array, -reach, reach).astype(held_as)


def bell_draw_with(own_key, shape, spread, reach, split, heavy, dtype=jnp.bfloat16):
    values = spread * jax.random.normal(own_key, shape, jnp.float32)
    if split:
        values = values * level_of(own_key, shape, split, -0.22, 0.18)
    return jnp.clip(strengthened(values, jax.random.fold_in(own_key, 3), *heavy), -reach, reach).astype(dtype)


def setup_inputs(seed: int = 0) -> dict:
    seeds = jax.random.split(jax.random.key(seed), 9)
    return {
        "train_gate": bell_draw_with(seeds[0], (D_MODEL, D_INNER), D_MODEL ** -0.5, 0.125, ((0, 4), (1, 8)), (0, 1, 8, 2.0), jnp.float32),
        "drift_gate": gaussian(seeds[1], (D_MODEL, D_INNER), D_MODEL ** -0.5, 0.09375, ((0, 4), (1, 8)), jnp.float32),
        "spread_gate": gaussian(seeds[2], (D_MODEL, D_INNER), D_MODEL ** -0.5, 0.09375, ((0, 4), (1, 8)), jnp.float32),
        "train_up": bell_draw_with(seeds[3], (D_MODEL, D_INNER), D_MODEL ** -0.5, 0.125, ((0, 4), (1, 8)), (0, 1, 8, 2.0), jnp.float32),
        "drift_up": gaussian(seeds[4], (D_MODEL, D_INNER), D_MODEL ** -0.5, 0.09375, ((0, 4), (1, 8)), jnp.float32),
        "spread_up": gaussian(seeds[5], (D_MODEL, D_INNER), D_MODEL ** -0.5, 0.09375, ((0, 4), (1, 8)), jnp.float32),
        "norm_train": jnp.clip(1.0 + 0.15 * jax.random.normal(seeds[6], (D_MODEL,), jnp.float32), 0.25, 1.75),
        "norm_step": jnp.clip(jax.random.uniform(seeds[7], (D_MODEL,), jnp.float32, -0.3, 0.3) * level_of(seeds[7], (D_MODEL,), ((0, 32),), -0.4, 0.0), -0.3, 0.3),
    }


learn_rate = 0.3
hold_rate = 0.9

def reference(train_gate, drift_gate, spread_gate, train_up, drift_up, spread_up, norm_train, norm_step):
    hold_gate = hold_rate * drift_gate + spread_gate
    whole_gate = train_gate - learn_rate * hold_gate
    hold_up = hold_rate * drift_up + spread_up
    whole_up = train_up - learn_rate * hold_up
    scale_gate = jnp.sqrt(lax.optimization_barrier(jnp.sum(whole_gate * whole_gate, axis=0)))
    serving_gate = (whole_gate / scale_gate).astype(jnp.bfloat16)
    scale_up = jnp.sqrt(lax.optimization_barrier(jnp.sum(whole_up * whole_up, axis=0)))
    serving_up = (whole_up / scale_up).astype(jnp.bfloat16)
    serve_norm = (norm_train + norm_step).astype(jnp.bfloat16)
    return (serving_gate, serving_up, scale_gate, scale_up, serve_norm, whole_gate, whole_up)
```

```python
import functools

import jax
import jax.numpy as jnp
from jax import lax
from jax.experimental import pallas as pl
from jax.experimental.pallas import tpu as pltpu
from jax.sharding import PartitionSpec as P

learn_rate = 0.3
hold_rate = 0.9
LANES = 128
SUB = 16
MESH = pl.DeviceIdType.MESH


def ring_order(n):
    side = int(round(n**0.5))
    if side * side != n or side % 2:
        return list(range(n))
    walk = [y * side for y in range(side)]
    for y in reversed(range(side)):
        columns = range(1, side) if (side - 1 - y) % 2 == 0 else reversed(range(1, side))
        walk += [y * side + x for x in columns]
    return walk


def pick(table, index):
    value = jnp.int32(table[0])
    for k in range(1, len(table)):
        value = jnp.where(index == k, jnp.int32(table[k]), value)
    return value


def groups_of(columns):
    first = min(LANES, columns // 4 // LANES * LANES)
    second = min(3 * LANES, columns // 3 // LANES * LANES)
    cuts = [0] + [c for c in (first, first + second) if c] + [columns]
    gate = [(0, a, b - a) for a, b in zip(cuts, cuts[1:]) if b > a]
    return gate + [(1, 0, columns)]


def middle(columns):
    return columns // (2 * SUB) * SUB


def gather_kernel(n, w, order, names, *refs):
    (tg, dg, sg, tu, du, su, nt, ns) = refs[:8]
    (out_g, out_u, whole_g, whole_u, right_piece, left_piece, scale_out, norm_out) = refs[8:16]
    (tv, dv, sv, nv, passed, sums, q, scale_buf, norm_in, norm_buf) = refs[16:26]
    (in_sem, put_sem, piece_sem, small_sem, sum_send, sum_recv) = refs[26:32]
    (ring_send, ring_recv, nf_send, nf_recv, nw_send, nw_recv) = refs[32:]
    f_axis, w_axis = names
    columns, rows = tg.shape
    groups = groups_of(columns)
    last = len(groups) - 1
    args = ((tg, dg, sg), (tu, du, su))
    outs, wholes = (out_g, out_u), (whole_g, whole_u)
    me = lax.axis_index(f_axis)
    mw = lax.axis_index(w_axis)
    half_ring = n // 2
    at = {d: i for i, d in enumerate(order)}
    right = pick([order[(at[d] + 1) % n] for d in range(n)], me)
    left = pick([order[(at[d] - 1) % n] for d in range(n)], me)
    cut = middle(columns)

    loads = {}

    def load(g):
        m, c0, cn = groups[g]
        loads[g] = [
            pltpu.make_async_copy(
                args[m][k].at[pl.ds(c0, cn)], buf.at[m, pl.ds(c0, cn)], in_sem.at[k]
            )
            for k, buf in enumerate((tv, dv, sv))
        ]
        for copy in loads[g]:
            copy.start()

    barrier = pltpu.get_barrier_semaphore()
    for k in range(1, n):
        pl.semaphore_signal(
            barrier, inc=1, device_id={f_axis: lax.rem(me + k, n)}, device_id_type=MESH
        )
    load(0)
    above, below = mw < w - 1, mw > 0

    @pl.when(above)
    def _():
        pl.semaphore_signal(barrier, inc=1, device_id={w_axis: mw + 1}, device_id_type=MESH)

    @pl.when(below)
    def _():
        pl.semaphore_signal(barrier, inc=1, device_id={w_axis: mw - 1}, device_id_type=MESH)

    norm_loads = [
        pltpu.make_async_copy(x, norm_in.at[k], small_sem.at[k]) for k, x in enumerate((nt, ns))
    ]
    for copy in norm_loads:
        copy.start()
    q[...] = jnp.zeros_like(q)

    def blocks(c0, cn, body):
        full = cn // LANES

        @pl.loop(0, full)
        def _(b):
            body(pl.multiple_of(c0 + b * LANES, LANES), LANES)

        if cn % LANES:
            body(c0 + full * LANES, cn % LANES)

    def step_block(m, c, cn):
        for r in range(0, cn, SUB):
            at_rows = pl.ds(c + r, SUB)
            part = None
            for l in range(0, rows, LANES):
                lanes = pl.ds(l, LANES)
                hold = hold_rate * dv[m, at_rows, lanes] + sv[m, at_rows, lanes]
                new = tv[m, at_rows, lanes] - learn_rate * hold
                tv[m, at_rows, lanes] = new
                part = new * new if part is None else part + new * new
            q[pl.ds(r, SUB), :] = part
        sums[m, me, :, pl.ds(c, LANES)] = jnp.sum(q[...].T, axis=0, keepdims=True)

    def narrow_block(m, c, cn):
        lanes = pl.ds(c, LANES)
        total = sums[m, 0, :, lanes]
        for k in range(1, n):
            total = total + sums[m, k, :, lanes]
        scale = jnp.sqrt(total)
        scale_buf[m, :, lanes] = scale
        q[...] = jnp.broadcast_to(scale, (LANES, LANES)).T
        for r in range(0, cn, SUB):
            at_rows = pl.ds(c + r, SUB)
            by = q[pl.ds(r, SUB), :]
            for l in range(0, rows, LANES):
                lanes = pl.ds(l, LANES)
                nv[m, at_rows, lanes] = (tv[m, at_rows, lanes] / by).astype(jnp.bfloat16)

    puts = []
    sends = []

    def exchange(g):
        m, c0, cn = groups[g]
        lanes = pl.ds(c0, -(-cn // LANES) * LANES)
        for k in range(1, n):
            copy = pltpu.make_async_remote_copy(
                src_ref=sums.at[m, me, :, lanes],
                dst_ref=sums.at[m, me, :, lanes],
                send_sem=sum_send.at[g, k - 1],
                recv_sem=sum_recv.at[g, k - 1],
                device_id={f_axis: lax.rem(me + k, n)},
                device_id_type=MESH,
            )
            copy.start()
            sends.append(copy)

    def exchanged(g):
        m, c0, cn = groups[g]
        lanes = pl.ds(c0, -(-cn // LANES) * LANES)
        for k in range(1, n):
            come = lax.rem(me - k + n, n)
            pltpu.make_async_remote_copy(
                src_ref=sums.at[m, come, :, lanes],
                dst_ref=sums.at[m, come, :, lanes],
                send_sem=sum_send.at[g, k - 1],
                recv_sem=sum_recv.at[g, k - 1],
                device_id={f_axis: come},
                device_id_type=MESH,
            ).wait_recv()

    def origin(s, way):
        shift = -s if way == 0 else s
        return pick([order[(at[d] + shift) % n] for d in range(n)], me)

    def block_of(m, c, cn, block):
        return outs[m].at[pl.ds(c, cn), pl.ds(pl.multiple_of(block * rows, LANES), rows)]

    def ring_copies(g, s, way, sent):
        m, c0, cn = groups[g]
        block = origin(s if sent else s + 1, way)
        parts = [(c0, cn, False)]
        if s == half_ring - 1:
            half = middle(cn)
            parts = [(c0, half, False) if way == 0 else (c0 + half, cn - half, False)]
        elif g == last and s == half_ring - 2:
            parts = [(0, cut, way == 0), (cut, columns - cut, way == 1)]
            if way == 1:
                parts.reverse()
        copies = []
        for p, (c, k, kept) in enumerate(parts):
            place = block_of(m, c, k, block)
            copies.append(
                pltpu.make_async_remote_copy(
                    src_ref=nv.at[m, pl.ds(c, k)] if s == 0 and sent else place,
                    dst_ref=passed.at[pl.ds(c, k)] if kept else place,
                    send_sem=ring_send.at[g * half_ring + s + p, way],
                    recv_sem=ring_recv.at[g * half_ring + s + p, way],
                    device_id={f_axis: right if way == 0 else left},
                    device_id_type=MESH,
                )
            )
        return copies

    def ring_start(g, s):
        for pair in zip(ring_copies(g, s, 0, True), ring_copies(g, s, 1, True)):
            for copy in pair:
                copy.start()

    def norm_spread(k):
        return pltpu.make_async_remote_copy(
            src_ref=norm_buf.at[me, mw],
            dst_ref=norm_buf.at[me, mw],
            send_sem=nf_send.at[k - 1],
            recv_sem=nf_recv.at[k - 1],
            device_id={f_axis: lax.rem(me + k, n)},
            device_id_type=MESH,
        )

    def norm_pass(k, up, sent):
        held = mw - k if up else mw + k
        if not sent:
            held = held - 1 if up else held + 1
        place = norm_buf.at[:, held]
        return pltpu.make_async_remote_copy(
            src_ref=place,
            dst_ref=place,
            send_sem=nw_send.at[int(up)],
            recv_sem=nw_recv.at[k, int(up)],
            device_id={w_axis: mw + 1 if up else mw - 1},
            device_id_type=MESH,
        )

    def norm_gather():
        for k in range(1, n):
            come = lax.rem(me - k + n, n)
            pltpu.make_async_remote_copy(
                src_ref=norm_buf.at[come, mw],
                dst_ref=norm_buf.at[come, mw],
                send_sem=nf_send.at[k - 1],
                recv_sem=nf_recv.at[k - 1],
                device_id={f_axis: come},
                device_id_type=MESH,
            ).wait_recv()
        for k in range(w - 1):
            steps = (
                (True, jnp.logical_and(above, mw >= k), jnp.logical_and(below, mw >= k + 1)),
                (
                    False,
                    jnp.logical_and(below, mw + k < w),
                    jnp.logical_and(above, mw + k + 1 < w),
                ),
            )
            for up, sending, _ in steps:

                @pl.when(sending)
                def _():
                    norm_pass(k, up, True).start()

            for up, sending, coming in steps:

                @pl.when(coming)
                def _():
                    norm_pass(k, up, False).wait_recv()

                @pl.when(sending)
                def _():
                    norm_pass(k, up, True).wait_send()

        put(norm_buf, norm_out, small_sem.at[2])

    def put(source, place, sem):
        copy = pltpu.make_async_copy(source, place, sem)
        copy.start()
        puts.append(copy)

    def step(g):
        m, c0, cn = groups[g]
        for copy in loads[g]:
            copy.wait()
        if g < last:
            load(g + 1)
        blocks(c0, cn, functools.partial(step_block, m))
        if g == 0:
            pl.semaphore_wait(barrier, n - 1 + above.astype(jnp.int32) + below.astype(jnp.int32))
        exchange(g)
        if g == 0:
            for copy in norm_loads:
                copy.wait()
            norm_buf[me, mw] = norm_in[0, 0] + norm_in[1, 0]
            for k in range(1, n):
                copy = norm_spread(k)
                copy.start()
                sends.append(copy)

    def narrow(g):
        m, c0, cn = groups[g]
        exchanged(g)
        blocks(c0, cn, functools.partial(narrow_block, m))

    def keep(g):
        m, c0, cn = groups[g]
        put(tv.at[m, pl.ds(c0, cn)], wholes[m].at[pl.ds(c0, cn)], put_sem.at[g, 0])
        put(nv.at[m, pl.ds(c0, cn)], block_of(m, c0, cn, me), put_sem.at[g, 1])

    def receive(g, s):
        for way in (0, 1):
            for copy in ring_copies(g, s, way, False):
                copy.wait_recv()

    def forward(g, s):
        if s + 1 < half_ring and (g, s + 1) != (last, half_ring - 1):
            ring_start(g, s + 1)
        if (g, s) == (last, half_ring - 2):
            ranges = ((0, cut, right_piece), (cut, columns - cut, left_piece))
            for way, (c, k, piece) in enumerate(ranges):
                source = passed.at[pl.ds(c, k)]
                put(source, piece, piece_sem.at[way, 0])
                put(source, block_of(1, c, k, origin(s + 1, way)), piece_sem.at[way, 1])

    yields = lax.rem(mw, 2) == 0

    step(0)
    for g in range(len(groups)):
        if g < last:
            step(g + 1)
        narrow(g)
        if g < last:
            ring_start(g, 0)
        if g:
            keep(g - 1)

    @pl.when(jnp.logical_not(yields))
    def _():
        ring_start(last, 0)

    keep(last)
    put(scale_buf, scale_out, small_sem.at[3])

    norm_gather()
    for g in range(last):
        receive(g, 0)

    @pl.when(yields)
    def _():
        ring_start(last, 0)

    for g in range(last):
        forward(g, 0)
    for s in range(half_ring):
        for g in range(len(groups)):
            if (g, s) != (last, half_ring - 1) and (s > 0 or g == last):
                receive(g, s)
                forward(g, s)
    for copy in sends:
        copy.wait_send()
    for s in range(half_ring):
        for g in range(len(groups)):
            if (g, s) != (last, half_ring - 1):
                for way in (0, 1):
                    for copy in ring_copies(g, s, way, True):
                        copy.wait_send()
    for copy in puts:
        copy.wait()


def copy_kernel(*refs):
    half = len(refs) // 2
    for source, place in zip(refs[:half], refs[half:]):
        place[...] = source[...]


def place_kernel(n, order, f_axis, right_far, left_far, _, out, sem):
    cut, rows = right_far.shape
    me = lax.axis_index(f_axis)
    at = {d: i for i, d in enumerate(order)}
    far = pick([order[(at[d] + n // 2) % n] for d in range(n)], me)
    lanes = pl.ds(pl.multiple_of(far * rows, LANES), rows)
    ranges = ((right_far, 0, cut), (left_far, cut, left_far.shape[0]))
    copies = [
        pltpu.make_async_copy(piece, out.at[pl.ds(c, k), lanes], sem.at[i])
        for i, (piece, c, k) in enumerate(ranges)
    ]
    for copy in copies:
        copy.start()
    for copy in copies:
        copy.wait()


def solution(mesh):
    names = mesh.axis_names
    n, w = mesh.shape["fsdp"], mesh.shape["width"]
    order = ring_order(n)

    def shards(tg, dg, sg, tu, du, su, nt, ns):
        rows, columns = tg.shape
        padded = -(-columns // LANES) * LANES
        length = nt.shape[0]
        wide = -(-length // LANES) * LANES

        def line(x):
            return jnp.pad(x, (0, wide - length)).reshape(1, 1, wide)

        groups = len(groups_of(columns))
        hbm = pl.BlockSpec(memory_space=pl.ANY)
        vmem = pl.BlockSpec(memory_space=pltpu.VMEM)
        dma = pltpu.SemaphoreType.DMA
        sent = 3 * 2 * columns * rows * 2
        cut = middle(columns)
        bf16 = jnp.bfloat16
        out_g, out_u, whole_g, whole_u, right_piece, left_piece, scales, norm = pl.pallas_call(
            functools.partial(gather_kernel, n, w, order, names),
            out_shape=(
                jax.ShapeDtypeStruct((columns, n * rows), bf16),
                jax.ShapeDtypeStruct((columns, n * rows), bf16),
                jax.ShapeDtypeStruct((columns, rows), jnp.float32),
                jax.ShapeDtypeStruct((columns, rows), jnp.float32),
                jax.ShapeDtypeStruct((cut, rows), bf16),
                jax.ShapeDtypeStruct((columns - cut, rows), bf16),
                jax.ShapeDtypeStruct((2, 1, padded), jnp.float32),
                jax.ShapeDtypeStruct((n, w, 1, wide), jnp.float32),
            ),
            in_specs=[hbm] * 8,
            out_specs=[hbm] * 8,
            scratch_shapes=[
                pltpu.VMEM((2, columns, rows), jnp.float32),
                pltpu.VMEM((2, columns, rows), jnp.float32),
                pltpu.VMEM((2, columns, rows), jnp.float32),
                pltpu.VMEM((2, columns, rows), bf16),
                pltpu.VMEM((columns, rows), bf16),
                pltpu.VMEM((2, n, 1, padded), jnp.float32),
                pltpu.VMEM((LANES, LANES), jnp.float32),
                pltpu.VMEM((2, 1, padded), jnp.float32),
                pltpu.VMEM((2, 1, 1, wide), jnp.float32),
                pltpu.VMEM((n, w, 1, wide), jnp.float32),
                dma((3,)),
                dma((groups, 2)),
                dma((2, 2)),
                dma((4,)),
                dma((groups, n - 1)),
                dma((groups, n - 1)),
                dma((groups * (n // 2) + 1, 2)),
                dma((groups * (n // 2) + 1, 2)),
                dma((n - 1,)),
                dma((n - 1,)),
                dma((2,)),
                dma((w - 1, 2)),
            ],
            compiler_params=pltpu.CompilerParams(
                collective_id=0, has_side_effects=True, vmem_limit_bytes=60 * 1024 * 1024
            ),
            cost_estimate=pl.CostEstimate(
                flops=20 * columns * rows, bytes_accessed=16 * sent, transcendentals=0
            ),
        )(tg.T, dg.T, sg.T, tu.T, du.T, su.T, line(nt), line(ns))
        right_far, left_far = (
            lax.ppermute(piece, "fsdp", [(order[i], order[(i + sign) % n]) for i in range(n)])
            for piece, sign in ((right_piece, 1), (left_piece, -1))
        )
        moved = (out_g, out_u, whole_g, whole_u)
        specs = [pl.BlockSpec((LANES, x.shape[1]), lambda i: (i, 0)) for x in moved]
        out_g, out_u, whole_g, whole_u = pl.pallas_call(
            copy_kernel,
            grid=(-(-columns // LANES),),
            out_shape=tuple(jax.ShapeDtypeStruct(x.shape, x.dtype) for x in moved),
            in_specs=specs,
            out_specs=specs,
            compiler_params=pltpu.CompilerParams(vmem_limit_bytes=60 * 1024 * 1024),
            cost_estimate=pl.CostEstimate(
                flops=0, bytes_accessed=2 * sum(x.size * x.dtype.itemsize for x in moved), transcendentals=0
            ),
        )(*moved)
        out_u = pl.pallas_call(
            functools.partial(place_kernel, n, order, "fsdp"),
            out_shape=jax.ShapeDtypeStruct(out_u.shape, out_u.dtype),
            in_specs=[vmem, vmem, hbm],
            out_specs=hbm,
            input_output_aliases={2: 0},
            scratch_shapes=[dma((2,))],
            compiler_params=pltpu.CompilerParams(vmem_limit_bytes=16 * 1024 * 1024),
            cost_estimate=pl.CostEstimate(
                flops=0, bytes_accessed=4 * columns * rows, transcendentals=0
            ),
        )(right_far, left_far, out_u)
        serve_norm = norm[..., :length].reshape(n * w * length).astype(jnp.bfloat16)
        return (
            out_g.T,
            out_u.T,
            scales[0, 0, :columns],
            scales[1, 0, :columns],
            serve_norm,
            whole_g.T,
            whole_u.T,
        )

    split = P("fsdp", "width")
    flat = P(("fsdp", "width"))
    return jax.shard_map(
        shards,
        mesh=mesh,
        in_specs=(split,) * 6 + (flat,) * 2,
        out_specs=(P(None, "width"), P(None, "width"), P("width"), P("width"), P(), split, split),
        check_vma=False,
    )
```

```python
import functools

import jax
import jax.numpy as jnp
from jax import lax
from jax.experimental import pallas as pl
from jax.experimental.pallas import tpu as pltpu
from jax.sharding import PartitionSpec as P

learn_rate = 0.3
hold_rate = 0.9
LANES = 128
SUB = 16
CHUNK = 352
RAW = 2 * SUB
MESH = pl.DeviceIdType.MESH


def ring_order(n):
    side = int(round(n**0.5))
    if side * side != n or side % 2:
        return list(range(n))
    walk = [y * side for y in range(side)]
    for y in reversed(range(side)):
        columns = range(1, side) if (side - 1 - y) % 2 == 0 else reversed(range(1, side))
        walk += [y * side + x for x in columns]
    return walk


def pick(table, index):
    value = jnp.int32(table[0])
    for k in range(1, len(table)):
        value = jnp.where(index == k, jnp.int32(table[k]), value)
    return value


def groups_of(columns):
    first = min(LANES, columns // 4 // LANES * LANES)
    second = min(3 * LANES, columns // 3 // LANES * LANES)
    cuts = [0] + [c for c in (first, first + second) if c] + [columns]
    gate = [(0, a, b - a) for a, b in zip(cuts, cuts[1:]) if b > a]
    return gate + [(1, 0, columns)]


def rings_of(columns):
    (m, c0, cn), *others = groups_of(columns)
    return [(m, c0, RAW), (m, c0 + RAW, cn - RAW), *others]


def middle(columns):
    return columns // (2 * SUB) * SUB


def tail_cut(columns):
    return middle(columns) + SUB


def pieces_of(columns):
    cut = tail_cut(columns)
    small = min(4 * SUB, cut // 2 // SUB * SUB)
    return [(0, cut - small), (cut, columns - cut - small), (cut - small, small), (columns - small, small)]


def gather_kernel(n, w, order, names, *refs):
    (tg, dg, sg, tu, du, su, nt, ns) = refs[:8]
    (out_g, out_u, whole_g, whole_u, scale_out, norm_out) = refs[8:14]
    pieces, refs = refs[14:18], refs[18:]
    (tv, dv, sv, nv, passed, sums, q, scale_buf, norm_in, norm_buf, raw_buf, near_buf) = refs[:12]
    (in_sem, put_sem, piece_sem, small_sem, sum_send, sum_recv) = refs[12:18]
    (ring_send, ring_recv, nf_send, nf_recv, nw_send, nw_recv) = refs[18:]
    f_axis, w_axis = names
    columns, rows = tg.shape
    groups = groups_of(columns)
    rings = rings_of(columns)
    last, end = len(groups) - 1, len(rings) - 1
    args = ((tg, dg, sg), (tu, du, su))
    outs, wholes = (out_g, out_u), (whole_g, whole_u)
    me = lax.axis_index(f_axis)
    mw = lax.axis_index(w_axis)
    half_ring = n // 2
    at = {d: i for i, d in enumerate(order)}
    right = pick([order[(at[d] + 1) % n] for d in range(n)], me)
    left = pick([order[(at[d] - 1) % n] for d in range(n)], me)
    cut = tail_cut(columns)

    loads = {}

    def load(g):
        m, c0, cn = groups[g]
        loads[g] = [
            pltpu.make_async_copy(
                args[m][k].at[pl.ds(c0, cn)], buf.at[m, pl.ds(c0, cn)], in_sem.at[k]
            )
            for k, buf in enumerate((tv, dv, sv))
        ]
        for copy in loads[g]:
            copy.start()

    barrier = pltpu.get_barrier_semaphore()
    for k in range(1, n):
        pl.semaphore_signal(
            barrier, inc=1, device_id={f_axis: lax.rem(me + k, n)}, device_id_type=MESH
        )
    load(0)
    above, below = mw < w - 1, mw > 0

    @pl.when(above)
    def _():
        pl.semaphore_signal(barrier, inc=1, device_id={w_axis: mw + 1}, device_id_type=MESH)

    @pl.when(below)
    def _():
        pl.semaphore_signal(barrier, inc=1, device_id={w_axis: mw - 1}, device_id_type=MESH)

    norm_loads = [
        pltpu.make_async_copy(x, norm_in.at[k], small_sem.at[k]) for k, x in enumerate((nt, ns))
    ]
    for copy in norm_loads:
        copy.start()
    q[...] = jnp.zeros_like(q)

    def blocks(c0, cn, body):
        full = cn // LANES

        @pl.loop(0, full)
        def _(b):
            body(pl.multiple_of(c0 + b * LANES, LANES), LANES)

        if cn % LANES:
            body(c0 + full * LANES, cn % LANES)

    def step_block(m, c, cn):
        for r in range(0, cn, SUB):
            at_rows = pl.ds(c + r, SUB)
            part = None
            for l in range(0, rows, LANES):
                lanes = pl.ds(l, LANES)
                hold = hold_rate * dv[m, at_rows, lanes] + sv[m, at_rows, lanes]
                new = tv[m, at_rows, lanes] - learn_rate * hold
                tv[m, at_rows, lanes] = new
                part = new * new if part is None else part + new * new
            q[pl.ds(r, SUB), :] = part
        sums[m, me, :, pl.ds(c, LANES)] = jnp.sum(q[...].T, axis=0, keepdims=True)

    def narrow_block(m, c, cn):
        lanes = pl.ds(c, LANES)
        total = sums[m, 0, :, lanes]
        for k in range(1, n):
            total = total + sums[m, k, :, lanes]
        scale = jnp.sqrt(total)
        scale_buf[m, :, lanes] = scale
        q[...] = jnp.broadcast_to(scale, (LANES, LANES)).T
        for r in range(0, cn, SUB):
            at_rows = pl.ds(c + r, SUB)
            by = q[pl.ds(r, SUB), :]
            for l in range(0, rows, LANES):
                lanes = pl.ds(l, LANES)
                nv[m, at_rows, lanes] = (tv[m, at_rows, lanes] / by).astype(jnp.bfloat16)

    puts = []
    sends = []

    def exchange(g):
        m, c0, cn = groups[g]
        lanes = pl.ds(c0, -(-cn // LANES) * LANES)
        for k in range(1, n):
            copy = pltpu.make_async_remote_copy(
                src_ref=sums.at[m, me, :, lanes],
                dst_ref=sums.at[m, me, :, lanes],
                send_sem=sum_send.at[g, k - 1],
                recv_sem=sum_recv.at[g, k - 1],
                device_id={f_axis: lax.rem(me + k, n)},
                device_id_type=MESH,
            )
            copy.start()
            sends.append(copy)

    def exchanged(g):
        m, c0, cn = groups[g]
        lanes = pl.ds(c0, -(-cn // LANES) * LANES)
        for k in range(1, n):
            come = lax.rem(me - k + n, n)
            pltpu.make_async_remote_copy(
                src_ref=sums.at[m, come, :, lanes],
                dst_ref=sums.at[m, come, :, lanes],
                send_sem=sum_send.at[g, k - 1],
                recv_sem=sum_recv.at[g, k - 1],
                device_id={f_axis: come},
                device_id_type=MESH,
            ).wait_recv()

    def origin(s, way):
        shift = -s if way == 0 else s
        return pick([order[(at[d] + shift) % n] for d in range(n)], me)

    def block_of(m, c, cn, block):
        return outs[m].at[pl.ds(c, cn), pl.ds(pl.multiple_of(block * rows, LANES), rows)]

    def ring_copies(g, s, way, sent):
        m, c0, cn = rings[g]
        block = origin(s if sent else s + 1, way)
        parts = [(c0, cn, False)]
        if s == half_ring - 1:
            half = middle(cn)
            parts = [(c0, half, False) if way == 0 else (c0 + half, cn - half, False)]
        elif g == end and s == half_ring - 2:
            parts = [(0, cut, way == 0), (cut, columns - cut, way == 1)]
            if way == 1:
                parts.reverse()
        copies = []
        for p, (c, k, kept) in enumerate(parts):
            place = block_of(m, c, k, block)
            source = nv.at[m, pl.ds(c, k)] if s == 0 and sent else place
            target = passed.at[pl.ds(c, k)] if kept else place
            if g == 0 and s == 0:
                source, target = tv.at[m, pl.ds(c, k)], raw_buf.at[way]
            elif g == 0 and s == 1 and sent:
                source = near_buf.at[way, pl.ds(c, k)]
            copies.append(
                pltpu.make_async_remote_copy(
                    src_ref=source,
                    dst_ref=target,
                    send_sem=ring_send.at[g * half_ring + s + p, way],
                    recv_sem=ring_recv.at[g * half_ring + s + p, way],
                    device_id={f_axis: right if way == 0 else left},
                    device_id_type=MESH,
                )
            )
        return copies

    def ring_start(g, s):
        for pair in zip(ring_copies(g, s, 0, True), ring_copies(g, s, 1, True)):
            for copy in pair:
                copy.start()

    def norm_spread(k):
        return pltpu.make_async_remote_copy(
            src_ref=norm_buf.at[me, mw],
            dst_ref=norm_buf.at[me, mw],
            send_sem=nf_send.at[k - 1],
            recv_sem=nf_recv.at[k - 1],
            device_id={f_axis: lax.rem(me + k, n)},
            device_id_type=MESH,
        )

    def norm_pass(k, up, sent):
        held = mw - k if up else mw + k
        if not sent:
            held = held - 1 if up else held + 1
        place = norm_buf.at[:, held]
        return pltpu.make_async_remote_copy(
            src_ref=place,
            dst_ref=place,
            send_sem=nw_send.at[int(up)],
            recv_sem=nw_recv.at[k, int(up)],
            device_id={w_axis: mw + 1 if up else mw - 1},
            device_id_type=MESH,
        )

    def norm_gather():
        for k in range(1, n):
            come = lax.rem(me - k + n, n)
            pltpu.make_async_remote_copy(
                src_ref=norm_buf.at[come, mw],
                dst_ref=norm_buf.at[come, mw],
                send_sem=nf_send.at[k - 1],
                recv_sem=nf_recv.at[k - 1],
                device_id={f_axis: come},
                device_id_type=MESH,
            ).wait_recv()
        for k in range(w - 1):
            steps = (
                (True, jnp.logical_and(above, mw >= k), jnp.logical_and(below, mw >= k + 1)),
                (
                    False,
                    jnp.logical_and(below, mw + k < w),
                    jnp.logical_and(above, mw + k + 1 < w),
                ),
            )
            for up, sending, _ in steps:

                @pl.when(sending)
                def _():
                    norm_pass(k, up, True).start()

            for up, sending, coming in steps:

                @pl.when(coming)
                def _():
                    norm_pass(k, up, False).wait_recv()

                @pl.when(sending)
                def _():
                    norm_pass(k, up, True).wait_send()

        put(norm_buf, norm_out, small_sem.at[2])

    def put(source, place, sem):
        copy = pltpu.make_async_copy(source, place, sem)
        copy.start()
        puts.append(copy)

    def step(g):
        m, c0, cn = groups[g]
        for copy in loads[g]:
            copy.wait()
        if g < last:
            load(g + 1)
        blocks(c0, cn, functools.partial(step_block, m))
        if g == 0:
            pl.semaphore_wait(barrier, n - 1 + above.astype(jnp.int32) + below.astype(jnp.int32))
        exchange(g)
        if g == 0:
            ring_start(0, 0)
            for copy in norm_loads:
                copy.wait()
            norm_buf[me, mw] = norm_in[0, 0] + norm_in[1, 0]
            for k in range(1, n):
                copy = norm_spread(k)
                copy.start()
                sends.append(copy)

    def narrow(g):
        m, c0, cn = groups[g]
        exchanged(g)
        blocks(c0, cn, functools.partial(narrow_block, m))

    def keep(g):
        m, c0, cn = groups[g]
        put(tv.at[m, pl.ds(c0, cn)], wholes[m].at[pl.ds(c0, cn)], put_sem.at[g, 0])
        put(nv.at[m, pl.ds(c0, cn)], block_of(m, c0, cn, me), put_sem.at[g, 1])

    def sent(g, s):
        for way in (0, 1):
            for copy in ring_copies(g, s, way, True):
                copy.wait_send()

    def receive(g, s):
        for way in (0, 1):
            for copy in ring_copies(g, s, way, False):
                copy.wait_recv()

    def narrow_near():
        q[...] = jnp.broadcast_to(scale_buf[0, :, pl.ds(0, LANES)], (LANES, LANES)).T
        for way in (0, 1):
            for r in range(0, RAW, SUB):
                at_rows = pl.ds(r, SUB)
                by = q[at_rows, :]
                for l in range(0, rows, LANES):
                    lanes = pl.ds(l, LANES)
                    near_buf[way, at_rows, lanes] = (raw_buf[way, at_rows, lanes] / by).astype(
                        jnp.bfloat16
                    )
            put(near_buf.at[way], block_of(0, 0, RAW, origin(1, way)), small_sem.at[4 + way])

    def forward(g, s):
        if s + 1 < half_ring and (g, s + 1) != (end, half_ring - 1):
            ring_start(g, s + 1)
        if (g, s) == (end, half_ring - 2):
            for i, ((c, k), piece) in enumerate(zip(pieces_of(columns), pieces)):
                put(passed.at[pl.ds(c, k)], piece, piece_sem.at[i])
            for way, (c, k) in enumerate(((0, cut), (cut, columns - cut))):
                near = block_of(1, c, k, origin(s + 1, way))
                put(passed.at[pl.ds(c, k)], near, piece_sem.at[len(pieces) + way])

    yields = lax.rem(mw, 2) == 0

    step(0)
    for g in range(len(groups)):
        if g < last:
            step(g + 1)
        narrow(g)
        if g == last - 1:

            @pl.when(yields)
            def _():
                sent(g, 0)

        if g < last:
            ring_start(g + 1, 0)
        if g:
            keep(g - 1)

    @pl.when(jnp.logical_not(yields))
    def _():
        ring_start(end, 0)

    keep(last)
    put(scale_buf, scale_out, small_sem.at[3])

    norm_gather()
    for g in range(end):
        receive(g, 0)
    narrow_near()

    @pl.when(yields)
    def _():
        ring_start(end, 0)

    for g in range(end):
        forward(g, 0)
    for s in range(half_ring):
        for g in range(len(rings)):
            if (g, s) != (end, half_ring - 1) and (s > 0 or g == end):
                receive(g, s)
                forward(g, s)
    for copy in sends:
        copy.wait_send()
    for s in range(half_ring):
        for g in range(len(rings)):
            if (g, s) not in ((end, half_ring - 1), (last - 1, 0)):
                sent(g, s)

    @pl.when(jnp.logical_not(yields))
    def _():
        sent(last - 1, 0)

    for copy in puts:
        copy.wait()


def far_lanes(n, order, f_axis, rows, ahead):
    me = lax.axis_index(f_axis)
    at = {d: i for i, d in enumerate(order)}
    block = pick([order[(at[d] + n // 2 + ahead) % n] for d in range(n)], me)
    return pl.ds(pl.multiple_of(block * rows, LANES), rows)


def chunks_of(columns):
    return [(c, min(CHUNK, columns - c)) for c in range(0, columns, CHUNK)]


def copy_kernel(n, order, f_axis, *refs):
    sources, places, held = refs[:4], refs[4:8], refs[8:11]
    come_sem, go_sem = refs[11:]
    columns, rows = sources[2].shape
    moves = []
    for c, k in chunks_of(columns):
        at_rows = pl.ds(c, k)
        moves += [(m + 2, (at_rows,), held[2].at[m, at_rows]) for m in range(2)]
        moves.append((0, (at_rows,), held[0].at[at_rows]))
        for b in range(1, n):
            moves.append((1, (at_rows, far_lanes(n, order, f_axis, rows, b)), held[1].at[b - 1, at_rows]))
    comes = [
        pltpu.make_async_copy(sources[m].at[where], buf, come_sem.at[i])
        for i, (m, where, buf) in enumerate(moves)
    ]
    goes = [
        pltpu.make_async_copy(buf, places[m].at[where], go_sem.at[i])
        for i, (m, where, buf) in enumerate(moves)
    ]
    for copy in comes:
        copy.start()
    for come, go in zip(comes, goes):
        come.wait()
        go.start()
    for copy in goes:
        copy.wait()


def place_kernel(n, order, f_axis, starts, *refs):
    pieces, out, sem = refs[: len(starts)], refs[-2], refs[-1]
    lanes = far_lanes(n, order, f_axis, pieces[0].shape[1], 0)
    copies = [
        pltpu.make_async_copy(piece, out.at[pl.ds(c, piece.shape[0]), lanes], sem.at[i])
        for i, (piece, c) in enumerate(zip(pieces, starts))
    ]
    for copy in copies:
        copy.start()
    for copy in copies:
        copy.wait()


def solution(mesh):
    names = mesh.axis_names
    n, w = mesh.shape["fsdp"], mesh.shape["width"]
    order = ring_order(n)

    def shards(tg, dg, sg, tu, du, su, nt, ns):
        rows, columns = tg.shape
        padded = -(-columns // LANES) * LANES
        length = nt.shape[0]
        wide = -(-length // LANES) * LANES

        def line(x):
            return jnp.pad(x, (0, wide - length)).reshape(1, 1, wide)

        groups = len(groups_of(columns))
        hbm = pl.BlockSpec(memory_space=pl.ANY)
        vmem = pl.BlockSpec(memory_space=pltpu.VMEM)
        dma = pltpu.SemaphoreType.DMA
        sent = 3 * 2 * columns * rows * 2
        pieces = pieces_of(columns)
        bf16 = jnp.bfloat16
        out_g, out_u, whole_g, whole_u, scales, norm, *handed = pl.pallas_call(
            functools.partial(gather_kernel, n, w, order, names),
            out_shape=(
                jax.ShapeDtypeStruct((columns, n * rows), bf16),
                jax.ShapeDtypeStruct((columns, n * rows), bf16),
                jax.ShapeDtypeStruct((columns, rows), jnp.float32),
                jax.ShapeDtypeStruct((columns, rows), jnp.float32),
                jax.ShapeDtypeStruct((2, 1, padded), jnp.float32),
                jax.ShapeDtypeStruct((n, w, 1, wide), jnp.float32),
                *(jax.ShapeDtypeStruct((k, rows), bf16) for _, k in pieces),
            ),
            in_specs=[hbm] * 8,
            out_specs=[hbm] * (6 + len(pieces)),
            scratch_shapes=[
                pltpu.VMEM((2, columns, rows), jnp.float32),
                pltpu.VMEM((2, columns, rows), jnp.float32),
                pltpu.VMEM((2, columns, rows), jnp.float32),
                pltpu.VMEM((2, columns, rows), bf16),
                pltpu.VMEM((columns, rows), bf16),
                pltpu.VMEM((2, n, 1, padded), jnp.float32),
                pltpu.VMEM((LANES, LANES), jnp.float32),
                pltpu.VMEM((2, 1, padded), jnp.float32),
                pltpu.VMEM((2, 1, 1, wide), jnp.float32),
                pltpu.VMEM((n, w, 1, wide), jnp.float32),
                pltpu.VMEM((2, RAW, rows), jnp.float32),
                pltpu.VMEM((2, RAW, rows), bf16),
                dma((3,)),
                dma((groups, 2)),
                dma((6,)),
                dma((6,)),
                dma((groups, n - 1)),
                dma((groups, n - 1)),
                dma(((groups + 1) * (n // 2) + 1, 2)),
                dma(((groups + 1) * (n // 2) + 1, 2)),
                dma((n - 1,)),
                dma((n - 1,)),
                dma((2,)),
                dma((w - 1, 2)),
            ],
            compiler_params=pltpu.CompilerParams(
                collective_id=0, has_side_effects=True, vmem_limit_bytes=60 * 1024 * 1024
            ),
            cost_estimate=pl.CostEstimate(
                flops=20 * columns * rows, bytes_accessed=16 * sent, transcendentals=0
            ),
        )(tg.T, dg.T, sg.T, tu.T, du.T, su.T, line(nt), line(ns))

        def travel(pair):
            return [
                lax.ppermute(piece, "fsdp", [(order[i], order[(i + sign) % n]) for i in range(n)])
                for piece, sign in zip(pair, (1, -1))
            ]

        far = travel(handed[:2])
        moved = (out_g, out_u, whole_g, whole_u)
        count = len(chunks_of(columns)) * (n + 2)
        out_g, out_u, whole_g, whole_u = pl.pallas_call(
            functools.partial(copy_kernel, n, order, "fsdp"),
            out_shape=tuple(jax.ShapeDtypeStruct(x.shape, x.dtype) for x in moved),
            in_specs=[hbm] * 4,
            out_specs=[hbm] * 4,
            scratch_shapes=[
                pltpu.VMEM((columns, n * rows), bf16),
                pltpu.VMEM((n - 1, columns, rows), bf16),
                pltpu.VMEM((2, columns, rows), jnp.float32),
                dma((count,)),
                dma((count,)),
            ],
            compiler_params=pltpu.CompilerParams(vmem_limit_bytes=60 * 1024 * 1024),
            cost_estimate=pl.CostEstimate(
                flops=0, bytes_accessed=2 * sum(x.size * x.dtype.itemsize for x in moved), transcendentals=0
            ),
        )(*moved)
        out_u, *rest = lax.optimization_barrier((out_u, *handed[2:]))
        far += travel(rest)
        for first in range(0, len(far), 2):
            landed = far[first : first + 2]
            out_u = pl.pallas_call(
                functools.partial(
                    place_kernel, n, order, "fsdp", [c for c, _ in pieces[first : first + 2]]
                ),
                out_shape=jax.ShapeDtypeStruct(out_u.shape, out_u.dtype),
                in_specs=[vmem, vmem, hbm],
                out_specs=hbm,
                input_output_aliases={2: 0},
                scratch_shapes=[dma((2,))],
                compiler_params=pltpu.CompilerParams(vmem_limit_bytes=16 * 1024 * 1024),
                cost_estimate=pl.CostEstimate(
                    flops=0, bytes_accessed=2 * sum(2 * x.size for x in landed), transcendentals=0
                ),
            )(*landed, out_u)
        serve_norm = norm[..., :length].reshape(n * w * length).astype(jnp.bfloat16)
        return (
            out_g.T,
            out_u.T,
            scales[0, 0, :columns],
            scales[1, 0, :columns],
            serve_norm,
            whole_g.T,
            whole_u.T,
        )

    split = P("fsdp", "width")
    flat = P(("fsdp", "width"))
    return jax.shard_map(
        shards,
        mesh=mesh,
        in_specs=(split,) * 6 + (flat,) * 2,
        out_specs=(P(None, "width"), P(None, "width"), P("width"), P("width"), P(), split, split),
        check_vma=False,
    )
```

```python
import functools

import jax
import jax.numpy as jnp
from jax import lax
from jax.experimental import pallas as pl
from jax.experimental.pallas import tpu as pltpu
from jax.sharding import PartitionSpec as P

learn_rate = 0.3
hold_rate = 0.9
LANES = 128
SUB = 16
CHUNK = 352
RAW = 2 * SUB
MESH = pl.DeviceIdType.MESH


def ring_order(n):
    side = int(round(n**0.5))
    if side * side != n or side % 2:
        return list(range(n))
    walk = [y * side for y in range(side)]
    for y in reversed(range(side)):
        columns = range(1, side) if (side - 1 - y) % 2 == 0 else reversed(range(1, side))
        walk += [y * side + x for x in columns]
    return walk


def pick(table, index):
    value = jnp.int32(table[0])
    for k in range(1, len(table)):
        value = jnp.where(index == k, jnp.int32(table[k]), value)
    return value


def groups_of(columns):
    first = min(LANES, columns // 4 // LANES * LANES)
    second = min(3 * LANES, columns // 3 // LANES * LANES)
    cuts = [0] + [c for c in (first, first + second) if c] + [columns]
    gate = [(0, a, b - a) for a, b in zip(cuts, cuts[1:]) if b > a]
    return gate + [(1, 0, columns)]


def rings_of(columns):
    (m, c0, cn), *others = groups_of(columns)
    return [(m, c0, RAW), (m, c0 + RAW, cn - RAW), *others]


def middle(columns):
    return columns // (2 * SUB) * SUB


def tail_cut(columns):
    return middle(columns)


def pieces_of(columns):
    cut = tail_cut(columns)
    small = min(4 * SUB, cut // 2 // SUB * SUB)
    return [(0, cut - small), (cut, columns - cut - small), (cut - small, small), (columns - small, small)]


def gather_kernel(n, w, order, names, *refs):
    (tg, dg, sg, tu, du, su, nt, ns) = refs[:8]
    (out_g, out_u, whole_g, whole_u, scale_out, norm_out) = refs[8:14]
    pieces, refs = refs[14:18], refs[18:]
    (tv, dv, sv, nv, passed, sums, q, scale_buf, norm_in, norm_buf, raw_buf, near_buf) = refs[:12]
    (in_sem, put_sem, piece_sem, small_sem, sum_send, sum_recv) = refs[12:18]
    (ring_send, ring_recv, nf_send, nf_recv, nw_send, nw_recv) = refs[18:]
    f_axis, w_axis = names
    columns, rows = tg.shape
    groups = groups_of(columns)
    rings = rings_of(columns)
    last, end = len(groups) - 1, len(rings) - 1
    args = ((tg, dg, sg), (tu, du, su))
    outs, wholes = (out_g, out_u), (whole_g, whole_u)
    me = lax.axis_index(f_axis)
    mw = lax.axis_index(w_axis)
    half_ring = n // 2
    at = {d: i for i, d in enumerate(order)}
    right = pick([order[(at[d] + 1) % n] for d in range(n)], me)
    left = pick([order[(at[d] - 1) % n] for d in range(n)], me)
    cut = tail_cut(columns)

    loads = {}

    def load(g):
        m, c0, cn = groups[g]
        loads[g] = [
            pltpu.make_async_copy(
                args[m][k].at[pl.ds(c0, cn)], buf.at[m, pl.ds(c0, cn)], in_sem.at[k]
            )
            for k, buf in enumerate((tv, dv, sv))
        ]
        for copy in loads[g]:
            copy.start()

    barrier = pltpu.get_barrier_semaphore()
    for k in range(1, n):
        pl.semaphore_signal(
            barrier, inc=1, device_id={f_axis: lax.rem(me + k, n)}, device_id_type=MESH
        )
    load(0)
    above, below = mw < w - 1, mw > 0

    @pl.when(above)
    def _():
        pl.semaphore_signal(barrier, inc=1, device_id={w_axis: mw + 1}, device_id_type=MESH)

    @pl.when(below)
    def _():
        pl.semaphore_signal(barrier, inc=1, device_id={w_axis: mw - 1}, device_id_type=MESH)

    norm_loads = [
        pltpu.make_async_copy(x, norm_in.at[k], small_sem.at[k]) for k, x in enumerate((nt, ns))
    ]
    for copy in norm_loads:
        copy.start()
    q[...] = jnp.zeros_like(q)

    def blocks(c0, cn, body):
        full = cn // LANES

        @pl.loop(0, full)
        def _(b):
            body(pl.multiple_of(c0 + b * LANES, LANES), LANES)

        if cn % LANES:
            body(c0 + full * LANES, cn % LANES)

    def step_block(m, c, cn):
        for r in range(0, cn, SUB):
            at_rows = pl.ds(c + r, SUB)
            part = None
            for l in range(0, rows, LANES):
                lanes = pl.ds(l, LANES)
                hold = hold_rate * dv[m, at_rows, lanes] + sv[m, at_rows, lanes]
                new = tv[m, at_rows, lanes] - learn_rate * hold
                tv[m, at_rows, lanes] = new
                part = new * new if part is None else part + new * new
            q[pl.ds(r, SUB), :] = part
        sums[m, me, :, pl.ds(c, LANES)] = jnp.sum(q[...].T, axis=0, keepdims=True)

    def narrow_block(m, c, cn):
        lanes = pl.ds(c, LANES)
        total = sums[m, 0, :, lanes]
        for k in range(1, n):
            total = total + sums[m, k, :, lanes]
        scale = jnp.sqrt(total)
        scale_buf[m, :, lanes] = scale
        q[...] = jnp.broadcast_to(scale, (LANES, LANES)).T
        for r in range(0, cn, SUB):
            at_rows = pl.ds(c + r, SUB)
            by = q[pl.ds(r, SUB), :]
            for l in range(0, rows, LANES):
                lanes = pl.ds(l, LANES)
                nv[m, at_rows, lanes] = (tv[m, at_rows, lanes] / by).astype(jnp.bfloat16)

    puts = []
    sends = []

    def exchange(g):
        m, c0, cn = groups[g]
        lanes = pl.ds(c0, -(-cn // LANES) * LANES)
        for k in range(1, n):
            copy = pltpu.make_async_remote_copy(
                src_ref=sums.at[m, me, :, lanes],
                dst_ref=sums.at[m, me, :, lanes],
                send_sem=sum_send.at[g, k - 1],
                recv_sem=sum_recv.at[g, k - 1],
                device_id={f_axis: lax.rem(me + k, n)},
                device_id_type=MESH,
            )
            copy.start()
            sends.append(copy)

    def exchanged(g):
        m, c0, cn = groups[g]
        lanes = pl.ds(c0, -(-cn // LANES) * LANES)
        for k in range(1, n):
            come = lax.rem(me - k + n, n)
            pltpu.make_async_remote_copy(
                src_ref=sums.at[m, come, :, lanes],
                dst_ref=sums.at[m, come, :, lanes],
                send_sem=sum_send.at[g, k - 1],
                recv_sem=sum_recv.at[g, k - 1],
                device_id={f_axis: come},
                device_id_type=MESH,
            ).wait_recv()

    def origin(s, way):
        shift = -s if way == 0 else s
        return pick([order[(at[d] + shift) % n] for d in range(n)], me)

    def block_of(m, c, cn, block):
        return outs[m].at[pl.ds(c, cn), pl.ds(pl.multiple_of(block * rows, LANES), rows)]

    def ring_copies(g, s, way, sent):
        m, c0, cn = rings[g]
        block = origin(s if sent else s + 1, way)
        parts = [(c0, cn, False)]
        if s == half_ring - 1:
            half = middle(cn)
            parts = [(c0, half, False) if way == 0 else (c0 + half, cn - half, False)]
        elif g == end and s == half_ring - 2:
            parts = [(0, cut, way == 0), (cut, columns - cut, way == 1)]
            if way == 1:
                parts.reverse()
        copies = []
        for p, (c, k, kept) in enumerate(parts):
            place = block_of(m, c, k, block)
            source = nv.at[m, pl.ds(c, k)] if s == 0 and sent else place
            target = passed.at[pl.ds(c, k)] if kept else place
            if g == 0 and s == 0:
                source, target = tv.at[m, pl.ds(c, k)], raw_buf.at[way]
            elif g == 0 and s == 1 and sent:
                source = near_buf.at[way, pl.ds(c, k)]
            copies.append(
                pltpu.make_async_remote_copy(
                    src_ref=source,
                    dst_ref=target,
                    send_sem=ring_send.at[g * half_ring + s + p, way],
                    recv_sem=ring_recv.at[g * half_ring + s + p, way],
                    device_id={f_axis: right if way == 0 else left},
                    device_id_type=MESH,
                )
            )
        return copies

    def ring_start(g, s):
        for pair in zip(ring_copies(g, s, 0, True), ring_copies(g, s, 1, True)):
            for copy in pair:
                copy.start()

    def norm_spread(k):
        return pltpu.make_async_remote_copy(
            src_ref=norm_buf.at[me, mw],
            dst_ref=norm_buf.at[me, mw],
            send_sem=nf_send.at[k - 1],
            recv_sem=nf_recv.at[k - 1],
            device_id={f_axis: lax.rem(me + k, n)},
            device_id_type=MESH,
        )

    def norm_pass(k, up, sent):
        held = mw - k if up else mw + k
        if not sent:
            held = held - 1 if up else held + 1
        place = norm_buf.at[:, held]
        return pltpu.make_async_remote_copy(
            src_ref=place,
            dst_ref=place,
            send_sem=nw_send.at[int(up)],
            recv_sem=nw_recv.at[k, int(up)],
            device_id={w_axis: mw + 1 if up else mw - 1},
            device_id_type=MESH,
        )

    def norm_gather():
        for k in range(1, n):
            come = lax.rem(me - k + n, n)
            pltpu.make_async_remote_copy(
                src_ref=norm_buf.at[come, mw],
                dst_ref=norm_buf.at[come, mw],
                send_sem=nf_send.at[k - 1],
                recv_sem=nf_recv.at[k - 1],
                device_id={f_axis: come},
                device_id_type=MESH,
            ).wait_recv()
        for k in range(w - 1):
            steps = (
                (True, jnp.logical_and(above, mw >= k), jnp.logical_and(below, mw >= k + 1)),
                (
                    False,
                    jnp.logical_and(below, mw + k < w),
                    jnp.logical_and(above, mw + k + 1 < w),
                ),
            )
            for up, sending, _ in steps:

                @pl.when(sending)
                def _():
                    norm_pass(k, up, True).start()

            for up, sending, coming in steps:

                @pl.when(coming)
                def _():
                    norm_pass(k, up, False).wait_recv()

                @pl.when(sending)
                def _():
                    norm_pass(k, up, True).wait_send()

        put(norm_buf, norm_out, small_sem.at[2])

    def put(source, place, sem):
        copy = pltpu.make_async_copy(source, place, sem)
        copy.start()
        puts.append(copy)

    def step(g):
        m, c0, cn = groups[g]
        for copy in loads[g]:
            copy.wait()
        if g < last:
            load(g + 1)
        blocks(c0, cn, functools.partial(step_block, m))
        if g == 0:
            pl.semaphore_wait(barrier, n - 1 + above.astype(jnp.int32) + below.astype(jnp.int32))
        exchange(g)
        if g == 0:
            ring_start(0, 0)
            for copy in norm_loads:
                copy.wait()
            norm_buf[me, mw] = norm_in[0, 0] + norm_in[1, 0]
            for k in range(1, n):
                copy = norm_spread(k)
                copy.start()
                sends.append(copy)

    def narrow(g):
        m, c0, cn = groups[g]
        exchanged(g)
        blocks(c0, cn, functools.partial(narrow_block, m))

    def keep(g):
        m, c0, cn = groups[g]
        put(tv.at[m, pl.ds(c0, cn)], wholes[m].at[pl.ds(c0, cn)], put_sem.at[g, 0])
        put(nv.at[m, pl.ds(c0, cn)], block_of(m, c0, cn, me), put_sem.at[g, 1])

    def receive(g, s):
        for way in (0, 1):
            for copy in ring_copies(g, s, way, False):
                copy.wait_recv()

    def narrow_near():
        q[...] = jnp.broadcast_to(scale_buf[0, :, pl.ds(0, LANES)], (LANES, LANES)).T
        for way in (0, 1):
            for r in range(0, RAW, SUB):
                at_rows = pl.ds(r, SUB)
                by = q[at_rows, :]
                for l in range(0, rows, LANES):
                    lanes = pl.ds(l, LANES)
                    near_buf[way, at_rows, lanes] = (raw_buf[way, at_rows, lanes] / by).astype(
                        jnp.bfloat16
                    )
            put(near_buf.at[way], block_of(0, 0, RAW, origin(1, way)), small_sem.at[4 + way])

    def forward(g, s):
        if s + 1 < half_ring and (g, s + 1) != (end, half_ring - 1):
            ring_start(g, s + 1)
        if (g, s) == (end, half_ring - 2):
            for i, ((c, k), piece) in enumerate(zip(pieces_of(columns), pieces)):
                put(passed.at[pl.ds(c, k)], piece, piece_sem.at[i])
            for way, (c, k) in enumerate(((0, cut), (cut, columns - cut))):
                near = block_of(1, c, k, origin(s + 1, way))
                put(passed.at[pl.ds(c, k)], near, piece_sem.at[len(pieces) + way])

    yields = lax.rem(mw, 2) == 1

    step(0)
    for g in range(len(groups)):
        if g < last:
            step(g + 1)
        narrow(g)
        if 0 < g < last:

            @pl.when(yields)
            def _():
                for before in (0, 1) if g == 1 else (g,):
                    receive(before, 0)

        if g < last:
            ring_start(g + 1, 0)
        if g:
            keep(g - 1)

    @pl.when(jnp.logical_not(yields))
    def _():
        ring_start(end, 0)

    keep(last)
    put(scale_buf, scale_out, small_sem.at[3])

    norm_gather()

    @pl.when(jnp.logical_not(yields))
    def _():
        for before in range(last):
            receive(before, 0)

    receive(last, 0)
    narrow_near()

    @pl.when(yields)
    def _():
        ring_start(end, 0)

    @pl.when(jnp.logical_not(yields))
    def _():
        for g in range(end):
            forward(g, 0)

    receive(end, 0)

    @pl.when(yields)
    def _():
        for g in range(end):
            forward(g, 0)

    forward(end, 0)
    for s in range(1, half_ring):
        for g in range(len(rings)):
            if (g, s) != (end, half_ring - 1):
                receive(g, s)
                forward(g, s)
    for copy in sends:
        copy.wait_send()
    for s in range(half_ring):
        for g in range(len(rings)):
            if (g, s) != (end, half_ring - 1):
                for way in (0, 1):
                    for copy in ring_copies(g, s, way, True):
                        copy.wait_send()
    for copy in puts:
        copy.wait()


def far_lanes(n, order, f_axis, rows, ahead):
    me = lax.axis_index(f_axis)
    at = {d: i for i, d in enumerate(order)}
    block = pick([order[(at[d] + n // 2 + ahead) % n] for d in range(n)], me)
    return pl.ds(pl.multiple_of(block * rows, LANES), rows)


def chunks_of(columns):
    return [(c, min(CHUNK, columns - c)) for c in range(0, columns, CHUNK)]


def copy_kernel(n, order, f_axis, *refs):
    sources, places, held = refs[:4], refs[4:8], refs[8:11]
    come_sem, go_sem = refs[11:]
    columns, rows = sources[2].shape
    moves = []
    for c, k in chunks_of(columns):
        at_rows = pl.ds(c, k)
        moves += [(m + 2, (at_rows,), held[2].at[m, at_rows]) for m in range(2)]
        moves.append((0, (at_rows,), held[0].at[at_rows]))
        for b in range(1, n):
            moves.append((1, (at_rows, far_lanes(n, order, f_axis, rows, b)), held[1].at[b - 1, at_rows]))
    comes = [
        pltpu.make_async_copy(sources[m].at[where], buf, come_sem.at[i])
        for i, (m, where, buf) in enumerate(moves)
    ]
    goes = [
        pltpu.make_async_copy(buf, places[m].at[where], go_sem.at[i])
        for i, (m, where, buf) in enumerate(moves)
    ]
    for copy in comes:
        copy.start()
    for come, go in zip(comes, goes):
        come.wait()
        go.start()
    for copy in goes:
        copy.wait()


def place_kernel(n, order, f_axis, starts, *refs):
    pieces, out, sem = refs[: len(starts)], refs[-2], refs[-1]
    lanes = far_lanes(n, order, f_axis, pieces[0].shape[1], 0)
    copies = [
        pltpu.make_async_copy(piece, out.at[pl.ds(c, piece.shape[0]), lanes], sem.at[i])
        for i, (piece, c) in enumerate(zip(pieces, starts))
    ]
    for copy in copies:
        copy.start()
    for copy in copies:
        copy.wait()


def solution(mesh):
    names = mesh.axis_names
    n, w = mesh.shape["fsdp"], mesh.shape["width"]
    order = ring_order(n)

    def shards(tg, dg, sg, tu, du, su, nt, ns):
        rows, columns = tg.shape
        padded = -(-columns // LANES) * LANES
        length = nt.shape[0]
        wide = -(-length // LANES) * LANES

        def line(x):
            return jnp.pad(x, (0, wide - length)).reshape(1, 1, wide)

        groups = len(groups_of(columns))
        hbm = pl.BlockSpec(memory_space=pl.ANY)
        vmem = pl.BlockSpec(memory_space=pltpu.VMEM)
        dma = pltpu.SemaphoreType.DMA
        sent = 3 * 2 * columns * rows * 2
        pieces = pieces_of(columns)
        bf16 = jnp.bfloat16
        out_g, out_u, whole_g, whole_u, scales, norm, *handed = pl.pallas_call(
            functools.partial(gather_kernel, n, w, order, names),
            out_shape=(
                jax.ShapeDtypeStruct((columns, n * rows), bf16),
                jax.ShapeDtypeStruct((columns, n * rows), bf16),
                jax.ShapeDtypeStruct((columns, rows), jnp.float32),
                jax.ShapeDtypeStruct((columns, rows), jnp.float32),
                jax.ShapeDtypeStruct((2, 1, padded), jnp.float32),
                jax.ShapeDtypeStruct((n, w, 1, wide), jnp.float32),
                *(jax.ShapeDtypeStruct((k, rows), bf16) for _, k in pieces),
            ),
            in_specs=[hbm] * 8,
            out_specs=[hbm] * (6 + len(pieces)),
            scratch_shapes=[
                pltpu.VMEM((2, columns, rows), jnp.float32),
                pltpu.VMEM((2, columns, rows), jnp.float32),
                pltpu.VMEM((2, columns, rows), jnp.float32),
                pltpu.VMEM((2, columns, rows), bf16),
                pltpu.VMEM((columns, rows), bf16),
                pltpu.VMEM((2, n, 1, padded), jnp.float32),
                pltpu.VMEM((LANES, LANES), jnp.float32),
                pltpu.VMEM((2, 1, padded), jnp.float32),
                pltpu.VMEM((2, 1, 1, wide), jnp.float32),
                pltpu.VMEM((n, w, 1, wide), jnp.float32),
                pltpu.VMEM((2, RAW, rows), jnp.float32),
                pltpu.VMEM((2, RAW, rows), bf16),
                dma((3,)),
                dma((groups, 2)),
                dma((6,)),
                dma((6,)),
                dma((groups, n - 1)),
                dma((groups, n - 1)),
                dma(((groups + 1) * (n // 2) + 1, 2)),
                dma(((groups + 1) * (n // 2) + 1, 2)),
                dma((n - 1,)),
                dma((n - 1,)),
                dma((2,)),
                dma((w - 1, 2)),
            ],
            compiler_params=pltpu.CompilerParams(
                collective_id=0, has_side_effects=True, vmem_limit_bytes=60 * 1024 * 1024
            ),
            cost_estimate=pl.CostEstimate(
                flops=20 * columns * rows, bytes_accessed=16 * sent, transcendentals=0
            ),
        )(tg.T, dg.T, sg.T, tu.T, du.T, su.T, line(nt), line(ns))

        def travel(pair):
            return [
                lax.ppermute(piece, "fsdp", [(order[i], order[(i + sign) % n]) for i in range(n)])
                for piece, sign in zip(pair, (1, -1))
            ]

        far = travel(handed[:2])
        moved = (out_g, out_u, whole_g, whole_u)
        count = len(chunks_of(columns)) * (n + 2)
        out_g, out_u, whole_g, whole_u = pl.pallas_call(
            functools.partial(copy_kernel, n, order, "fsdp"),
            out_shape=tuple(jax.ShapeDtypeStruct(x.shape, x.dtype) for x in moved),
            in_specs=[hbm] * 4,
            out_specs=[hbm] * 4,
            scratch_shapes=[
                pltpu.VMEM((columns, n * rows), bf16),
                pltpu.VMEM((n - 1, columns, rows), bf16),
                pltpu.VMEM((2, columns, rows), jnp.float32),
                dma((count,)),
                dma((count,)),
            ],
            compiler_params=pltpu.CompilerParams(vmem_limit_bytes=60 * 1024 * 1024),
            cost_estimate=pl.CostEstimate(
                flops=0, bytes_accessed=2 * sum(x.size * x.dtype.itemsize for x in moved), transcendentals=0
            ),
        )(*moved)
        out_u, *rest = lax.optimization_barrier((out_u, *handed[2:]))
        far += travel(rest)
        for first in range(0, len(far), 2):
            landed = far[first : first + 2]
            out_u = pl.pallas_call(
                functools.partial(
                    place_kernel, n, order, "fsdp", [c for c, _ in pieces[first : first + 2]]
                ),
                out_shape=jax.ShapeDtypeStruct(out_u.shape, out_u.dtype),
                in_specs=[vmem, vmem, hbm],
                out_specs=hbm,
                input_output_aliases={2: 0},
                scratch_shapes=[dma((2,))],
                compiler_params=pltpu.CompilerParams(vmem_limit_bytes=16 * 1024 * 1024),
                cost_estimate=pl.CostEstimate(
                    flops=0, bytes_accessed=2 * sum(2 * x.size for x in landed), transcendentals=0
                ),
            )(*landed, out_u)
        serve_norm = norm[..., :length].reshape(n * w * length).astype(jnp.bfloat16)
        return (
            out_g.T,
            out_u.T,
            scales[0, 0, :columns],
            scales[1, 0, :columns],
            serve_norm,
            whole_g.T,
            whole_u.T,
        )

    split = P("fsdp", "width")
    flat = P(("fsdp", "width"))
    return jax.shard_map(
        shards,
        mesh=mesh,
        in_specs=(split,) * 6 + (flat,) * 2,
        out_specs=(P(None, "width"), P(None, "width"), P("width"), P("width"), P(), split, split),
        check_vma=False,
    )
```
